256 devices in a mesh: band: 32 (over y_lo, z, core), slab: 8 (over x, y_hi).
Axes of the slice: x: 4, y: 4 (y_hi: 2, y_lo: 2; y = y_hi * 2 + y_lo), z: 8, core: 2. Of those that a mesh axis runs over, the one named last changes fastest.
Arguments:
- orbitals: bfloat16 [64, 128, 4096], P('band', 'slab'), may hold values from -6 to 6
- occupation: bfloat16 [64], P('band'), may hold values from 0.25 to 1
Outputs:
- exchange_field: float32 [64, 128, 4096], P('band', 'slab')
The draws below stay inside these ranges and needn't reach their ends.
All inputs are finite; a program needn't handle non-finite values.
Results may differ from the reference program's by a relative error of at most 0.001.
Values may be sent and summed in bfloat16 or wider, within the bound.
No kernel may reach another device: no remote copies, remote signals or barrier semaphores. Data moves between devices by JAX's collectives and lax.ppermute only.
A program may use at most 64 MiB of HBM per device.

```python
import math
import jax
import jax.numpy as jnp
from jax import lax

ORB_DEV = 2
NY = 64
NZ = 64
STEPS = 3
ORBITALS = 64
NX = 128
N_BAND = 32


def levels(own_key, dims, split, least, top_value):
    loudness = 1.0
    for axis_at, shards_of in split:
        steps = jax.random.uniform(jax.random.fold_in(jax.random.fold_in(own_key, 6), axis_at), (shards_of,), jnp.float32, least / len(split), top_value / len(split))
        loudness = loudness * jnp.repeat(jnp.exp(steps), dims[axis_at] // shards_of).reshape((-1,) + (1,) * (len(dims) - 1 - axis_at))
    return loudness


def centred(rng, shape, deviation, limit, shards=(), held_as=jnp.bfloat16):
    array = jax.random.normal(rng, shape, jnp.float32) * deviation
    if len(shards) > 0:
        array = levels(rng, shape, shards, -0.22, 0.18) * array
    return jnp.clip(array, min=-limit, max=limit).astype(held_as)


def setup_inputs(seed: int = 0) -> dict:
    key_list = jax.random.split(jax.random.key(seed), 3)
    return {
        "orbitals": centred(key_list[0], (ORBITALS, NX, NY * NZ), 1.0, 6.0, ((0, 32), (1, 8))),
        "occupation": jnp.clip(jnp.exp(math.log(1.0) - 1.3862944 * jax.random.uniform(key_list[1], (ORBITALS,), jnp.float32) ** levels(key_list[1], (ORBITALS,), ((0, 32),), -0.2, 0.2)), 0.25, 1.0).astype(jnp.bfloat16),
    }


screening = 0.5
ratio_mid = (12.0 + 2.0 * screening) / 12.0
root_term = math.sqrt(ratio_mid * ratio_mid - 1.0)
decay_ratio = ratio_mid - root_term
coeff_zero = 1.0 / (6.0 * root_term)
coeff_one = -2.0 * decay_ratio * coeff_zero
coeff_two = 2.0 * decay_ratio * decay_ratio * coeff_zero

def cross_sum(values):
    rest = ((0, 0),) * (values.ndim - 1)
    padded_y = jnp.pad(values, rest + ((NZ, NZ),))
    along_y = padded_y[..., 2 * NZ:] + padded_y[..., :-2 * NZ]
    narrow = jnp.pad(values, rest + ((1, 1),))
    column = jnp.arange(values.shape[-1], dtype=jnp.int32) % NZ
    left_side = jnp.where(column != 0, narrow[..., :-2], 0.0)
    right_side = jnp.where(column != NZ - 1, narrow[..., 2:], 0.0)
    return along_y + (left_side + right_side)

def neighbour(values):
    padded = jnp.pad(values, ((0, 0), (0, 0), (1, 1), (0, 0)))
    return padded[:, :, 2:] + padded[:, :, :-2] + cross_sum(values)

def reference(orbitals, occupation):
    cells = NY * NZ
    orbital_grid = orbitals.astype(jnp.float32).reshape(N_BAND, ORB_DEV, NX, cells)
    occupied = occupation.astype(jnp.float32).reshape(N_BAND, ORB_DEV)

    def one_block(block_index):
        own_block = lax.dynamic_index_in_dim(orbital_grid, block_index, 0, keepdims=False)
        running = jnp.zeros((ORB_DEV, NX, cells), jnp.float32)
        for visit in range(STEPS + 1):
            source_block = ((block_index - visit) % N_BAND).astype(jnp.int32)
            visitor = lax.dynamic_index_in_dim(orbital_grid, source_block, 0, keepdims=False)
            weights = lax.dynamic_index_in_dim(occupied, source_block, 0, keepdims=False)
            density = own_block[:, None] * visitor[None]
            first_term = -neighbour(density) / 6.0
            second_term = -neighbour(first_term) / 3.0 - density
            potential = coeff_zero * density + coeff_one * first_term + coeff_two * second_term
            running = running - lax.optimization_barrier(jnp.sum(weights[None, :, None, None] * visitor[None] * potential, axis=1))
        return running
    result = lax.map(one_block, jnp.arange(N_BAND, dtype=jnp.int32))
    return result.reshape(ORBITALS, NX, cells)
```

```python
import math

import jax
import jax.numpy as jnp
from jax import lax
from jax.experimental import pallas as pl
from jax.experimental.pallas import tpu as pltpu
from jax.sharding import PartitionSpec as P

NZ = 64
STEPS = 3
LANES = 128
UNROLL = 4

screening = 0.5
ratio_mid = (12.0 + 2.0 * screening) / 12.0
root_term = math.sqrt(ratio_mid * ratio_mid - 1.0)
decay_ratio = ratio_mid - root_term
coeff_zero = 1.0 / (6.0 * root_term)
coeff_one = -2.0 * decay_ratio * coeff_zero
coeff_two = 2.0 * decay_ratio * decay_ratio * coeff_zero

lead = coeff_two / 18.0
slope = (-coeff_one / 6.0) / lead
base = (coeff_zero - coeff_two) / lead

PAIRS = ((0, 0), (1, 1), (0, 1), (1, 0))


def visit_kernel(own_ref, own_halo_ref, visitor_ref, halo_ref, *rest):
    running_ref = rest[0] if len(rest) == 6 else None
    out_ref, rho, rho_y, mid, mid_y = rest[-5:]
    groups = own_ref.shape[2] // LANES
    shape = (8, LANES)
    lane = lax.broadcasted_iota(jnp.int32, shape, 1)
    row = lax.broadcasted_iota(jnp.int32, shape, 0)
    low = lane < NZ
    has_left = lane % NZ != 0
    has_right = lane % NZ != NZ - 1
    zero = jnp.zeros(shape, jnp.float32)

    def lanes_by(v, k):
        return pltpu.roll(v, k % LANES, axis=1)

    def rows_by(v, k):
        return pltpu.roll(v, k % 8, axis=0)

    own_tail = own_halo_ref[:, groups * LANES :].astype(jnp.float32)
    tail = halo_ref[:, groups * LANES :].astype(jnp.float32)
    inside = own_tail > 0.0
    weight = []
    for j in range(2):
        w = jnp.maximum(tail[2 * j : 2 * j + 1], tail[4 + 2 * j : 5 + 2 * j])
        weight.append(jnp.broadcast_to(w * -lead, shape))

    def columns(g):
        return pl.ds(pl.multiple_of(g * LANES, LANES), LANES)

    def both(ref, i, g):
        v = ref[i, :, columns(g)].astype(jnp.float32)
        return v[:8], v[8:]

    for k in range(10):
        rho_y[0, k] = zero
        rho_y[groups + 1, k] = zero
    for k in range(8):
        mid_y[0, k] = zero
        mid_y[groups + 1, k] = zero

    def transverse(v, about_y, at, k):
        left = jnp.where(has_left, lanes_by(v, 1), 0.0)
        right = jnp.where(has_right, lanes_by(v, -1), 0.0)
        across = jnp.where(low, about_y[at - 1, k], about_y[at + 1, k])
        return (about_y[at, k] + across) + (left + right)

    def along(v0, v1, edge_down, edge_up):
        a0, a1 = rows_by(v0, 1), rows_by(v1, 1)
        b0, b1 = rows_by(v0, -1), rows_by(v1, -1)
        first, last = row == 0, row == 7
        n0 = jnp.where(first, edge_down, a0) + jnp.where(last, b1, b0)
        n1 = jnp.where(first, a0, a1) + jnp.where(last, edge_up, b1)
        return n0, n1, a0, b1

    def step_rho(g):
        own = [both(own_ref, i, g) for i in range(2)]
        vis = [both(visitor_ref, j, g) for j in range(2)]
        oh = own_halo_ref[:, columns(g)].astype(jnp.float32)
        vh = halo_ref[:, columns(g)].astype(jnp.float32)
        swapped = jnp.where(row % 4 < 2, rows_by(vh, -2), rows_by(vh, 2))
        vals = []
        for i, j in PAIRS:
            vals += [own[i][0] * vis[j][0], own[i][1] * vis[j][1]]
        vals += [oh * vh, oh * swapped]
        for k, v in enumerate(vals):
            rho[g, k] = v
            rho_y[g + 1, k] = lanes_by(v, NZ)

    def step_mid(g):
        for half in range(2):
            h = rho[g, 8 + half]
            up1, dn1 = rows_by(h, 1), rows_by(h, -1)
            up3, dn3 = rows_by(h, 3), rows_by(h, -3)
            pa, pb = 4 * half, 4 * half + 2
            va0, va1 = rho[g, pa], rho[g, pa + 1]
            vb0, vb1 = rho[g, pb], rho[g, pb + 1]
            na0, na1, first_a, _ = along(va0, va1, dn1, up3)
            nb0, nb1, _, last_b = along(vb0, vb1, dn3, up1)
            body = jnp.where(row == 1, first_a, jnp.where(row == 3, rows_by(vb0, 3), jnp.where(row == 4, rows_by(va1, -3), last_b)))
            nh = jnp.where(row < 4, up1, dn1) + body
            for k, v, n in ((pa, va0, na0), (pa + 1, va1, na1), (pb, vb0, nb0), (pb + 1, vb1, nb1)):
                m = v * slope + (n + transverse(v, rho_y, g + 1, k))
                mid[g, k] = m
                mid_y[g + 1, k] = lanes_by(m, NZ)
            m = h * slope + (nh + transverse(h, rho_y, g + 1, 8 + half))
            mid[g, 8 + half] = jnp.where(inside, m, 0.0)

    def step_out(g):
        vis = [both(visitor_ref, j, g) for j in range(2)]
        scaled = [(weight[j] * vis[j][0], weight[j] * vis[j][1]) for j in range(2)]
        total = [[None, None], [None, None]]
        for half in range(2):
            h = mid[g, 8 + half]
            up1, dn1 = rows_by(h, 1), rows_by(h, -1)
            up3, dn3 = rows_by(h, 3), rows_by(h, -3)
            for at, down, up in ((2 * half, dn1, up3), (2 * half + 1, dn3, up1)):
                i, j = PAIRS[at]
                v = (mid[g, 2 * at], mid[g, 2 * at + 1])
                n = along(*v, down, up)[:2]
                for e in range(2):
                    k = 2 * at + e
                    pot = rho[g, k] * base + (n[e] + transverse(v[e], mid_y, g + 1, k))
                    term = scaled[j][e] * pot
                    total[i][e] = term if total[i][e] is None else total[i][e] + term
        for i in range(2):
            for e in range(2):
                t = total[i][e]
                if running_ref is not None:
                    t = t + running_ref[i, 8 * e : 8 * e + 8, columns(g)]
                out_ref[i, 8 * e : 8 * e + 8, columns(g)] = t

    def sweep(step):
        def body(n, carry):
            for k in range(UNROLL):
                step(n * UNROLL + k)
            return carry

        lax.fori_loop(0, groups // UNROLL, body, 0)

    sweep(step_rho)
    sweep(step_mid)
    sweep(step_out)


def visit(own, own_halo, visitor, halo, running):
    groups = own.shape[2] // LANES
    operands = [own, own_halo, visitor, halo] + ([] if running is None else [running])
    vmem = pl.BlockSpec(memory_space=pltpu.VMEM)
    return pl.pallas_call(
        visit_kernel,
        out_shape=jax.ShapeDtypeStruct(own.shape, jnp.float32),
        in_specs=[vmem] * len(operands),
        out_specs=vmem,
        scratch_shapes=[
            pltpu.VMEM((groups, 10, 8, LANES), jnp.float32),
            pltpu.VMEM((groups + 2, 10, 8, LANES), jnp.float32),
            pltpu.VMEM((groups, 10, 8, LANES), jnp.float32),
            pltpu.VMEM((groups + 2, 8, 8, LANES), jnp.float32),
        ],
        input_output_aliases={} if running is None else {4: 0},
        name="visit",
    )(*operands)


def shifted(array, by):
    size = lax.axis_size("band")
    return lax.ppermute(array, "band", [(i, (i + by) % size) for i in range(size)])


def per_device(orbitals, occupation):
    size = lax.axis_size("slab")
    up = [(i, i + 1) for i in range(size - 1)]
    down = [(j, i) for i, j in up]
    planes = orbitals.shape[1]
    bodies = [orbitals, shifted(orbitals, 1), shifted(orbitals, 2)]
    bodies.append(shifted(bodies[2], 1))
    tail = jnp.broadcast_to(occupation[:, None, None], (2, 2, LANES))

    def edge(at):
        planes_at = lax.slice_in_dim(orbitals, at, at + 2, axis=1)
        return jnp.concatenate([planes_at, tail], axis=2).reshape(4, -1)

    before = lax.ppermute(edge(planes - 2), "slab", up)
    after = lax.ppermute(edge(0), "slab", down)
    halo = jnp.concatenate([before, after], axis=0)
    halos = [halo] + [shifted(halo, s) for s in range(1, STEPS + 1)]
    running = None
    for s in range(STEPS + 1):
        running = visit(orbitals, halo, bodies[s], halos[s], running)
    return running


def solution(mesh):
    return jax.shard_map(
        per_device,
        mesh=mesh,
        in_specs=(P("band", "slab", None), P("band")),
        out_specs=P("band", "slab", None),
        check_vma=False,
    )
```

```python
import math

import jax
import jax.numpy as jnp
from jax import lax
from jax.experimental import pallas as pl
from jax.experimental.pallas import tpu as pltpu
from jax.sharding import PartitionSpec as P


NZ = 64
LANES = 128
UNROLL_RHO = 8
UNROLL_MID = 16
UNROLL_OUT = 16

screening = 0.5
ratio_mid = (12.0 + 2.0 * screening) / 12.0
root_term = math.sqrt(ratio_mid * ratio_mid - 1.0)
decay_ratio = ratio_mid - root_term
coeff_zero = 1.0 / (6.0 * root_term)
coeff_one = -2.0 * decay_ratio * coeff_zero
coeff_two = 2.0 * decay_ratio * decay_ratio * coeff_zero

lead = coeff_two / 18.0
slope = (-coeff_one / 6.0) / lead
base = (coeff_zero - coeff_two) / lead

SHAPE = (8, LANES)
PAIRS = ((0, 0), (1, 1), (0, 1), (1, 0))


def lanes_by(v, k):
    return pltpu.roll(v, k % LANES, axis=1)


def rows_by(v, k):
    return pltpu.roll(v, k % 8, axis=0)


def iotas():
    return lax.broadcasted_iota(jnp.int32, SHAPE, 0), lax.broadcasted_iota(jnp.int32, SHAPE, 1)


def columns(g):
    return pl.ds(pl.multiple_of(g * LANES, LANES), LANES)


def planes_of(ref, i, g):
    v = ref[i, :, columns(g)].astype(jnp.float32)
    return v[:8], v[8:]


def at_row(at, e, by=0):
    return pl.ds(24 * at + 8 + 8 * e + by, 8)


def sweep(step, groups, unroll):
    def body(n, carry):
        for k in range(unroll):
            step(n * unroll + k)
        return carry

    lax.fori_loop(0, groups // unroll, body, 0)


def transverse(v, about_y, at, k, masks):
    low, has_left, has_right = masks
    left = jnp.where(has_left, lanes_by(v, 1), 0.0)
    right = jnp.where(has_right, lanes_by(v, -1), 0.0)
    across = jnp.where(low, about_y[at - 1, k], about_y[at + 1, k])
    return (about_y[at, k] + across) + (left + right)


def lane_masks(lane):
    return lane < NZ, lane % NZ != 0, lane % NZ != NZ - 1


def prepare_kernel(orbitals_ref, occupation_ref, wide_ref, first_ref, second_ref, *, even_of):
    cells = orbitals_ref.shape[2]
    planes = orbitals_ref.shape[1]
    wide_ref[:, :, :cells] = orbitals_ref[...]
    even = even_of()
    row = lax.broadcasted_iota(jnp.int32, (4, LANES), 0)
    weights = [occupation_ref[j].astype(jnp.float32) for j in range(2)]
    for j in range(2):
        wide_ref[j, :, cells:] = jnp.full((planes, LANES), weights[j], jnp.float32).astype(jnp.bfloat16)
    tail = jnp.where(row < 2, weights[0], weights[1]).astype(jnp.bfloat16)
    first_ref[:, cells:] = tail
    second_ref[:, cells:] = tail

    def step(g):
        v = [orbitals_ref[j, :, columns(g)].astype(jnp.float32) for j in range(2)]

        def rows(a, b):
            return jnp.concatenate([v[0][a : a + 1], v[0][b : b + 1], v[1][a : a + 1], v[1][b : b + 1]], axis=0)

        high, leading = rows(planes - 1, planes - 2), rows(1, 0)
        first_ref[:, columns(g)] = jnp.where(even, high, leading).astype(jnp.bfloat16)
        second_ref[:, columns(g)] = jnp.where(even, leading, high).astype(jnp.bfloat16)

    sweep(step, cells // LANES, 8)


def visit_kernel(own_ref, visitor_ref, *rest):
    running_ref = rest[0] if len(rest) == 4 else None
    out_ref, rho, mid = rest[-3:]
    groups = out_ref.shape[2] // LANES
    lane = iotas()[1]
    high, has_left, has_right = lane >= NZ, lane % NZ != 0, lane % NZ != NZ - 1
    zero = jnp.zeros(SHAPE, jnp.float32)
    weight = []
    for j in range(2):
        w = visitor_ref[j, :, groups * LANES :].astype(jnp.float32)
        weight.append(w[:8] * -lead)
    for ref in (rho, mid):
        for at in range(4):
            for e in range(2):
                ref[0, at_row(at, e), :] = zero
                ref[groups + 1, at_row(at, e), :] = zero

    def stencil(ref, g, at, e, v):
        left = jnp.where(has_left, lanes_by(v, 1), 0.0)
        right = jnp.where(has_right, lanes_by(v, -1), 0.0)
        rows = at_row(at, e)
        about = lanes_by(v + jnp.where(high, ref[g, rows, :], ref[g + 2, rows, :]), NZ)
        x = ref[g + 1, at_row(at, e, -1), :] + ref[g + 1, at_row(at, e, 1), :]
        return (x + about) + (left + right)

    def step_rho(g):
        own = [planes_of(own_ref, i, g) for i in range(2)]
        vis = [planes_of(visitor_ref, j, g) for j in range(2)]
        for n in range(5):
            rho[g + 1, pl.ds(24 * n, 8), :] = zero
            mid[g + 1, pl.ds(24 * n, 8), :] = zero
        for at, (i, j) in enumerate(PAIRS):
            for e in range(2):
                rho[g + 1, at_row(at, e), :] = own[i][e] * vis[j][e]

    def step_mid(g):
        for at in range(4):
            for e in range(2):
                v = rho[g + 1, at_row(at, e), :]
                mid[g + 1, at_row(at, e), :] = v * slope + stencil(rho, g, at, e, v)

    def step_out(g):
        vis = [planes_of(visitor_ref, j, g) for j in range(2)]
        for i in range(2):
            for e in range(2):
                total = None
                for at in range(4):
                    if PAIRS[at][0] == i:
                        v = mid[g + 1, at_row(at, e), :]
                        pot = rho[g + 1, at_row(at, e), :] * base + stencil(mid, g, at, e, v)
                        j = PAIRS[at][1]
                        term = (weight[j] * vis[j][e]) * pot
                        total = term if total is None else total + term
                if running_ref is not None:
                    total = total + running_ref[i, 8 * e : 8 * e + 8, columns(g)]
                out_ref[i, 8 * e : 8 * e + 8, columns(g)] = total

    sweep(step_rho, groups, UNROLL_RHO)
    sweep(step_mid, groups, UNROLL_MID)
    sweep(step_out, groups, UNROLL_OUT)


def edge_kernel(own_ref, own_halo_ref, *rest):
    out_ref, rho, rho_y = rest[-3:]
    running_ref = rest[-4]
    visitors = rest[: (len(rest) - 4) // 2]
    halos = rest[(len(rest) - 4) // 2 : -4]
    groups = out_ref.shape[2] // LANES
    row, lane = iotas()
    masks = lane_masks(lane)
    zero = jnp.zeros(SHAPE, jnp.float32)
    inside = own_halo_ref[:, groups * LANES :].astype(jnp.float32) > 0.0
    nearest = (row == 0) | (row == 2) | (row == 5) | (row == 7)
    near_inside = nearest & inside
    even_row = row % 2 == 0
    upper = row % 4 < 2

    def swap(v):
        return jnp.where(upper, rows_by(v, -2), rows_by(v, 2))

    def edges(ref, g):
        a0, a1 = planes_of(ref, 0, g)
        b0, b1 = planes_of(ref, 1, g)
        return jnp.where(row < 2, a0, jnp.where(row < 4, rows_by(b0, 2), jnp.where(row < 6, rows_by(a1, -2), b1)))

    weight = []
    for ref in visitors:
        w0 = ref[0, :, groups * LANES :].astype(jnp.float32)[:8]
        w1 = ref[1, :, groups * LANES :].astype(jnp.float32)[:8]
        weight.append(jnp.where(upper, w0, w1) * -lead)
    for k in range(2 * len(visitors)):
        rho_y[0, k] = zero
        rho_y[groups + 1, k] = zero

    def step_rho(g):
        oh = own_halo_ref[:, columns(g)].astype(jnp.float32)
        for n, ref in enumerate(halos):
            vh = ref[:, columns(g)].astype(jnp.float32)
            for k, v in ((2 * n, oh * vh), (2 * n + 1, oh * swap(vh))):
                rho[g, k] = v
                rho_y[g + 1, k] = lanes_by(v, NZ)

    def step_out(g):
        oe = edges(own_ref, g)
        total = None
        for n, ref in enumerate(visitors):
            ve = edges(ref, g)
            we = ve * weight[n]
            for k, ve, we in ((2 * n, ve, we), (2 * n + 1, swap(ve), swap(we))):
                v = rho[g, k]
                beside = jnp.where(even_row, rows_by(v, -1), rows_by(v, 1))
                t = transverse(v, rho_y, g + 1, k, masks)
                t = jnp.where(nearest, v * slope + (t + t), 0.0) + jnp.where(near_inside, oe * ve, 0.0)
                term = we * (beside + t)
                total = term if total is None else total + term
        for i in range(2):
            low_planes = running_ref[i, :8, columns(g)]
            out_ref[i, :8, columns(g)] = low_planes + jnp.where(row < 2, total if i == 0 else rows_by(total, -2), 0.0)
            high_planes = running_ref[i, 8:, columns(g)]
            out_ref[i, 8:, columns(g)] = high_planes + jnp.where(row >= 6, rows_by(total, 2) if i == 0 else total, 0.0)

    sweep(step_rho, groups, 32)
    sweep(step_out, groups, 16)


VMEM = pl.BlockSpec(memory_space=pltpu.VMEM)


def in_vmem(x):
    return pltpu.with_memory_space_constraint(x, pltpu.VMEM)


def prepare(orbitals, occupation, even_of):
    cells = orbitals.shape[2]
    return pl.pallas_call(
        lambda *refs: prepare_kernel(*refs, even_of=even_of),
        out_shape=[
            pltpu.VMEM((*orbitals.shape[:2], cells + LANES), orbitals.dtype),
            pltpu.VMEM((4, cells + LANES), orbitals.dtype),
            pltpu.VMEM((4, cells + LANES), orbitals.dtype),
        ],
        in_specs=[VMEM, pl.BlockSpec(memory_space=pltpu.SMEM)],
        out_specs=[VMEM] * 3,
        name="prepare",
    )(orbitals, occupation)


def visit(own, visitor, running):
    shape = (*own.shape[:2], own.shape[2] - LANES)
    groups = shape[2] // LANES
    operands = [in_vmem(x) for x in (own, visitor) + (() if running is None else (running,))]
    held = pltpu.VMEM((groups + 2, 104, LANES), jnp.float32)
    return pl.pallas_call(
        visit_kernel,
        out_shape=pltpu.VMEM(shape, jnp.float32),
        in_specs=[VMEM] * len(operands),
        out_specs=VMEM,
        scratch_shapes=[held, held],
        name="visit",
    )(*operands)


def finish(own, own_halo, visitors, halos, running):
    groups = running.shape[2] // LANES
    count = 2 * len(visitors)
    operands = [in_vmem(x) for x in (own, own_halo, *visitors, *halos, running)]
    return pl.pallas_call(
        edge_kernel,
        out_shape=jax.ShapeDtypeStruct(running.shape, jnp.float32),
        in_specs=[VMEM] * len(operands),
        out_specs=VMEM,
        scratch_shapes=[
            pltpu.VMEM((groups, count, *SHAPE), jnp.float32),
            pltpu.VMEM((groups + 2, count, *SHAPE), jnp.float32),
        ],
        name="finish",
    )(*operands)


def from_two_back(array):
    size = lax.axis_size("band")
    return lax.ppermute(array, "band", [(i, (i + 2) % size) for i in range(size)])


def across_pair_and_three(array):
    size = lax.axis_size("band")
    return lax.ppermute(array, "band", [(i, (i + 1 + 2 * (i % 2)) % size) for i in range(size)])


def swapped_in_pair(array):
    size = lax.axis_size("band")
    return lax.ppermute(array, "band", [(i, i ^ 1) for i in range(size)])


def per_device(orbitals, occupation):
    size = lax.axis_size("slab")
    even = lax.axis_index("slab") % 2 == 0
    wide, first, second = prepare(orbitals, occupation, lambda: lax.axis_index("slab") % 2 == 0)
    beside_second = lax.ppermute(second, "slab", [(i, ((i - 1) ^ 1) + 1) for i in range(1, size - 1)])
    beside_first = lax.ppermute(first, "slab", [(i, i ^ 1) for i in range(size)])
    two_back = from_two_back(wide)
    other = across_pair_and_three(wide)
    swapped = swapped_in_pair(two_back)
    halo = jnp.concatenate([jnp.where(even, beside_second, beside_first), jnp.where(even, beside_first, beside_second)], axis=0)
    halo_two = from_two_back(halo)
    halo_other = across_pair_and_three(halo)
    halo_swapped = swapped_in_pair(halo_two)
    running = visit(wide, wide, None)
    running = visit(wide, two_back, running)
    running = visit(wide, swapped, running)
    running = visit(wide, other, running)
    return finish(wide, halo, (wide, two_back, swapped, other), (halo, halo_two, halo_swapped, halo_other), running)


def solution(mesh):
    return jax.shard_map(
        per_device,
        mesh=mesh,
        in_specs=(P("band", "slab", None), P("band")),
        out_specs=P("band", "slab", None),
        check_vma=False,
    )
```

```python
import math

import jax
import jax.numpy as jnp
from jax import lax
from jax.experimental import pallas as pl
from jax.experimental.pallas import tpu as pltpu
from jax.sharding import PartitionSpec as P


NZ = 64
LANES = 128
UNROLL_RHO = 8
CHUNK = 32

screening = 0.5
ratio_mid = (12.0 + 2.0 * screening) / 12.0
root_term = math.sqrt(ratio_mid * ratio_mid - 1.0)
decay_ratio = ratio_mid - root_term
coeff_zero = 1.0 / (6.0 * root_term)
coeff_one = -2.0 * decay_ratio * coeff_zero
coeff_two = 2.0 * decay_ratio * decay_ratio * coeff_zero

lead = coeff_two / 18.0
slope = (-coeff_one / 6.0) / lead
base = (coeff_zero - coeff_two) / lead

SHAPE = (8, LANES)
PAIRS = ((0, 0), (1, 1), (0, 1), (1, 0))


def lanes_by(v, k):
    return pltpu.roll(v, k % LANES, axis=1)


def rows_by(v, k):
    return pltpu.roll(v, k % 8, axis=0)


def iotas():
    return lax.broadcasted_iota(jnp.int32, SHAPE, 0), lax.broadcasted_iota(jnp.int32, SHAPE, 1)


def columns(g):
    return pl.ds(pl.multiple_of(g * LANES, LANES), LANES)


def planes_of(ref, i, g):
    v = ref[i, :, columns(g)].astype(jnp.float32)
    return v[:8], v[8:]


def at_row(at, e, by=0):
    return pl.ds(24 * at + 8 + 8 * e + by, 8)


def sweep(step, groups, unroll):
    def body(n, carry):
        for k in range(unroll):
            step(n * unroll + k)
        return carry

    lax.fori_loop(0, groups // unroll, body, 0)


def transverse(v, about_y, at, k, masks):
    low, has_left, has_right = masks
    left = jnp.where(has_left, lanes_by(v, 1), 0.0)
    right = jnp.where(has_right, lanes_by(v, -1), 0.0)
    across = jnp.where(low, about_y[at - 1, k], about_y[at + 1, k])
    return (about_y[at, k] + across) + (left + right)


def lane_masks(lane):
    return lane < NZ, lane % NZ != 0, lane % NZ != NZ - 1


def prepare_kernel(orbitals_ref, occupation_ref, wide_ref, first_ref, second_ref, *, even_of):
    cells = orbitals_ref.shape[2]
    planes = orbitals_ref.shape[1]
    wide_ref[:, :, :cells] = orbitals_ref[...]
    even = even_of()
    row = lax.broadcasted_iota(jnp.int32, (4, LANES), 0)
    weights = [occupation_ref[j].astype(jnp.float32) for j in range(2)]
    for j in range(2):
        wide_ref[j, :, cells:] = jnp.full((planes, LANES), weights[j], jnp.float32).astype(jnp.bfloat16)
    tail = jnp.where(row < 2, weights[0], weights[1]).astype(jnp.bfloat16)
    first_ref[:, cells:] = tail
    second_ref[:, cells:] = tail

    def step(g):
        v = [orbitals_ref[j, :, columns(g)].astype(jnp.float32) for j in range(2)]

        def rows(a, b):
            return jnp.concatenate([v[0][a : a + 1], v[0][b : b + 1], v[1][a : a + 1], v[1][b : b + 1]], axis=0)

        high, leading = rows(planes - 1, planes - 2), rows(1, 0)
        first_ref[:, columns(g)] = jnp.where(even, high, leading).astype(jnp.bfloat16)
        second_ref[:, columns(g)] = jnp.where(even, leading, high).astype(jnp.bfloat16)

    sweep(step, cells // LANES, 8)


def neighbour_table():
    size = (2 * LANES, 2 * LANES)
    a, b = (lax.broadcasted_iota(jnp.int32, size, d) for d in range(2))
    apart = jnp.abs(a - b)
    near = (apart == NZ) | ((apart == 1) & (a // NZ == b // NZ))
    return jnp.where(near, 1.0, 0.0).astype(jnp.bfloat16)


def visit_kernel(*refs):
    first = len(refs) == 6
    own_ref, visitor_ref = refs[:2]
    if first:
        out_ref, table_ref, rho, mid = refs[2:]
        table_ref[...] = neighbour_table()
    else:
        running_ref, table_ref, out_ref, rho, mid = refs[2:]
    groups = out_ref.shape[2] // LANES
    low = iotas()[1] < NZ
    zero = jnp.zeros(SHAPE, jnp.float32)
    weight = []
    for j in range(2):
        w = visitor_ref[j, :, groups * LANES :].astype(jnp.float32)
        weight.append(w[:8] * -lead)
    for ref in (rho, mid):
        for at in range(4):
            for e in range(2):
                ref[0, at_row(at, e), :] = zero
                ref[groups + 1, at_row(at, e), :] = zero

    def stencils(ref, g0, count):
        rows = []
        for q in range(0, count, 2):
            for at in range(4):
                both = [ref[g0 + q + 1 + h, pl.ds(24 * at + 8, 16), :] for h in range(2)]
                rows.append(jnp.concatenate(both, axis=1))
        v = jnp.concatenate(rows, axis=0)
        coarse = v.astype(jnp.bfloat16)
        fine = (v - coarse.astype(jnp.float32)).astype(jnp.bfloat16)
        table = table_ref[...]
        inner = jnp.dot(coarse, table, preferred_element_type=jnp.float32)
        inner = inner + jnp.dot(fine, table, preferred_element_type=jnp.float32)
        result = {}
        for q in range(0, count, 2):
            for at in range(4):
                for e in range(2):
                    g = g0 + q + 1
                    rows = at_row(at, e)
                    outer = lanes_by(jnp.where(low, ref[g + 2, rows, :], ref[g - 1, rows, :]), NZ)
                    for h in range(2):
                        x = ref[g + h, at_row(at, e, -1), :] + ref[g + h, at_row(at, e, 1), :]
                        r = 32 * q + 16 * at + 8 * e
                        yz = inner[r : r + 8, LANES * h : LANES * h + LANES]
                        edge = jnp.where(low if h == 0 else ~low, outer, 0.0)
                        result[q + h, at, e] = (x + edge) + yz
        return result

    def step_rho(g):
        own = [planes_of(own_ref, i, g) for i in range(2)]
        vis = [planes_of(visitor_ref, j, g) for j in range(2)]
        for n in range(5):
            rho[g + 1, pl.ds(24 * n, 8), :] = zero
            mid[g + 1, pl.ds(24 * n, 8), :] = zero
        for at, (i, j) in enumerate(PAIRS):
            for e in range(2):
                rho[g + 1, at_row(at, e), :] = own[i][e] * vis[j][e]

    def step_mid(n):
        g0 = n * CHUNK
        nb = stencils(rho, g0, CHUNK)
        for (k, at, e), s in nb.items():
            mid[g0 + k + 1, at_row(at, e), :] = rho[g0 + k + 1, at_row(at, e), :] * slope + s

    def step_out(n):
        g0 = n * CHUNK
        nb = stencils(mid, g0, CHUNK)
        for k in range(CHUNK):
            g = g0 + k
            vis = [planes_of(visitor_ref, j, g) for j in range(2)]
            for i in range(2):
                for e in range(2):
                    total = None
                    for at in range(4):
                        if PAIRS[at][0] == i:
                            pot = rho[g + 1, at_row(at, e), :] * base + nb[k, at, e]
                            j = PAIRS[at][1]
                            term = (weight[j] * vis[j][e]) * pot
                            total = term if total is None else total + term
                    if not first:
                        total = total + running_ref[i, 8 * e : 8 * e + 8, columns(g)]
                    out_ref[i, 8 * e : 8 * e + 8, columns(g)] = total

    sweep(step_rho, groups, UNROLL_RHO)
    sweep(step_mid, groups // CHUNK, 1)
    sweep(step_out, groups // CHUNK, 1)


def edge_kernel(own_ref, own_halo_ref, *rest):
    out_ref, rho, rho_y = rest[-3:]
    running_ref = rest[-4]
    visitors = rest[: (len(rest) - 4) // 2]
    halos = rest[(len(rest) - 4) // 2 : -4]
    groups = out_ref.shape[2] // LANES
    row, lane = iotas()
    masks = lane_masks(lane)
    zero = jnp.zeros(SHAPE, jnp.float32)
    inside = own_halo_ref[:, groups * LANES :].astype(jnp.float32) > 0.0
    nearest = (row == 0) | (row == 2) | (row == 5) | (row == 7)
    near_inside = nearest & inside
    even_row = row % 2 == 0
    upper = row % 4 < 2

    def swap(v):
        return jnp.where(upper, rows_by(v, -2), rows_by(v, 2))

    def edges(ref, g):
        a0, a1 = planes_of(ref, 0, g)
        b0, b1 = planes_of(ref, 1, g)
        return jnp.where(row < 2, a0, jnp.where(row < 4, rows_by(b0, 2), jnp.where(row < 6, rows_by(a1, -2), b1)))

    weight = []
    for ref in visitors:
        w0 = ref[0, :, groups * LANES :].astype(jnp.float32)[:8]
        w1 = ref[1, :, groups * LANES :].astype(jnp.float32)[:8]
        weight.append(jnp.where(upper, w0, w1) * -lead)
    for k in range(2 * len(visitors)):
        rho_y[0, k] = zero
        rho_y[groups + 1, k] = zero

    def step_rho(g):
        oh = own_halo_ref[:, columns(g)].astype(jnp.float32)
        for n, ref in enumerate(halos):
            vh = ref[:, columns(g)].astype(jnp.float32)
            for k, v in ((2 * n, oh * vh), (2 * n + 1, oh * swap(vh))):
                rho[g, k] = v
                rho_y[g + 1, k] = lanes_by(v, NZ)

    def step_out(g):
        oe = edges(own_ref, g)
        total = None
        for n, ref in enumerate(visitors):
            ve = edges(ref, g)
            we = ve * weight[n]
            for k, ve, we in ((2 * n, ve, we), (2 * n + 1, swap(ve), swap(we))):
                v = rho[g, k]
                beside = jnp.where(even_row, rows_by(v, -1), rows_by(v, 1))
                t = transverse(v, rho_y, g + 1, k, masks)
                t = jnp.where(nearest, v * slope + (t + t), 0.0) + jnp.where(near_inside, oe * ve, 0.0)
                term = we * (beside + t)
                total = term if total is None else total + term
        for i in range(2):
            low_planes = running_ref[i, :8, columns(g)]
            out_ref[i, :8, columns(g)] = low_planes + jnp.where(row < 2, total if i == 0 else rows_by(total, -2), 0.0)
            high_planes = running_ref[i, 8:, columns(g)]
            out_ref[i, 8:, columns(g)] = high_planes + jnp.where(row >= 6, rows_by(total, 2) if i == 0 else total, 0.0)

    sweep(step_rho, groups, 32)
    sweep(step_out, groups, 16)


VMEM = pl.BlockSpec(memory_space=pltpu.VMEM)


def in_vmem(x):
    return pltpu.with_memory_space_constraint(x, pltpu.VMEM)


def prepare(orbitals, occupation, even_of):
    cells = orbitals.shape[2]
    return pl.pallas_call(
        lambda *refs: prepare_kernel(*refs, even_of=even_of),
        out_shape=[
            pltpu.VMEM((*orbitals.shape[:2], cells + LANES), orbitals.dtype),
            pltpu.VMEM((4, cells + LANES), orbitals.dtype),
            pltpu.VMEM((4, cells + LANES), orbitals.dtype),
        ],
        in_specs=[VMEM, pl.BlockSpec(memory_space=pltpu.SMEM)],
        out_specs=[VMEM] * 3,
        name="prepare",
    )(orbitals, occupation)


def visit(own, visitor, running=None, table=None):
    shape = (*own.shape[:2], own.shape[2] - LANES)
    groups = shape[2] // LANES
    first = running is None
    operands = [in_vmem(x) for x in (own, visitor) + (() if first else (running, table))]
    held = pltpu.VMEM((groups + 2, 104, LANES), jnp.float32)
    out = pltpu.VMEM(shape, jnp.float32)
    return pl.pallas_call(
        visit_kernel,
        out_shape=[out, pltpu.VMEM((2 * LANES, 2 * LANES), jnp.bfloat16)] if first else out,
        in_specs=[VMEM] * len(operands),
        out_specs=[VMEM] * 2 if first else VMEM,
        scratch_shapes=[held, held],
        name="visit",
    )(*operands)


def finish(own, own_halo, visitors, halos, running):
    groups = running.shape[2] // LANES
    count = 2 * len(visitors)
    operands = [in_vmem(x) for x in (own, own_halo, *visitors, *halos, running)]
    return pl.pallas_call(
        edge_kernel,
        out_shape=jax.ShapeDtypeStruct(running.shape, jnp.float32),
        in_specs=[VMEM] * len(operands),
        out_specs=VMEM,
        scratch_shapes=[
            pltpu.VMEM((groups, count, *SHAPE), jnp.float32),
            pltpu.VMEM((groups + 2, count, *SHAPE), jnp.float32),
        ],
        name="finish",
    )(*operands)


def from_two_back(array):
    size = lax.axis_size("band")
    return lax.ppermute(array, "band", [(i, (i + 2) % size) for i in range(size)])


def across_pair_and_three(array):
    size = lax.axis_size("band")
    return lax.ppermute(array, "band", [(i, (i + 1 + 2 * (i % 2)) % size) for i in range(size)])


def swapped_in_pair(array):
    size = lax.axis_size("band")
    return lax.ppermute(array, "band", [(i, i ^ 1) for i in range(size)])


def per_device(orbitals, occupation):
    size = lax.axis_size("slab")
    even = lax.axis_index("slab") % 2 == 0
    wide, first, second = prepare(orbitals, occupation, lambda: lax.axis_index("slab") % 2 == 0)
    beside_second = lax.ppermute(second, "slab", [(i, ((i - 1) ^ 1) + 1) for i in range(1, size - 1)])
    beside_first = lax.ppermute(first, "slab", [(i, i ^ 1) for i in range(size)])
    two_back = from_two_back(wide)
    other = across_pair_and_three(wide)
    swapped = swapped_in_pair(two_back)
    halo = jnp.concatenate([jnp.where(even, beside_second, beside_first), jnp.where(even, beside_first, beside_second)], axis=0)
    halo_two = from_two_back(halo)
    halo_other = across_pair_and_three(halo)
    halo_swapped = swapped_in_pair(halo_two)
    running, table = visit(wide, wide)
    running = visit(wide, two_back, running, table)
    running = visit(wide, swapped, running, table)
    running = visit(wide, other, running, table)
    return finish(wide, halo, (wide, two_back, swapped, other), (halo, halo_two, halo_swapped, halo_other), running)


def solution(mesh):
    return jax.shard_map(
        per_device,
        mesh=mesh,
        in_specs=(P("band", "slab", None), P("band")),
        out_specs=P("band", "slab", None),
        check_vma=False,
    )
```

```python
import math

import jax
import jax.numpy as jnp
from jax import lax
from jax.experimental import pallas as pl
from jax.experimental.pallas import tpu as pltpu
from jax.sharding import PartitionSpec as P


NZ = 64
LANES = 128
UNROLL_RHO = 8
CHUNK = 32

screening = 0.5
ratio_mid = (12.0 + 2.0 * screening) / 12.0
root_term = math.sqrt(ratio_mid * ratio_mid - 1.0)
decay_ratio = ratio_mid - root_term
coeff_zero = 1.0 / (6.0 * root_term)
coeff_one = -2.0 * decay_ratio * coeff_zero
coeff_two = 2.0 * decay_ratio * decay_ratio * coeff_zero

lead = coeff_two / 18.0
slope = (-coeff_one / 6.0) / lead
base = (coeff_zero - coeff_two) / lead

SHAPE = (8, LANES)
PAIRS = ((0, 0), (1, 1), (0, 1), (1, 0))


def lanes_by(v, k):
    return pltpu.roll(v, k % LANES, axis=1)


def rows_by(v, k):
    return pltpu.roll(v, k % 8, axis=0)


def iotas():
    return lax.broadcasted_iota(jnp.int32, SHAPE, 0), lax.broadcasted_iota(jnp.int32, SHAPE, 1)


def columns(g):
    return pl.ds(pl.multiple_of(g * LANES, LANES), LANES)


def planes_of(ref, i, g):
    v = ref[i, :, columns(g)].astype(jnp.float32)
    return v[:8], v[8:]


def at_row(at, e, by=0):
    return pl.ds(24 * at + 8 + 8 * e + by, 8)


def sweep(step, groups, unroll):
    def body(n, carry):
        for k in range(unroll):
            step(n * unroll + k)
        return carry

    lax.fori_loop(0, groups // unroll, body, 0)


def prepare_kernel(orbitals_ref, occupation_ref, wide_ref, first_ref, second_ref, *, even_of):
    cells = orbitals_ref.shape[2]
    planes = orbitals_ref.shape[1]
    wide_ref[:, :, :cells] = orbitals_ref[...]
    even = even_of()
    row = lax.broadcasted_iota(jnp.int32, (4, LANES), 0)
    weights = [occupation_ref[j].astype(jnp.float32) for j in range(2)]
    for j in range(2):
        wide_ref[j, :, cells:] = jnp.full((planes, LANES), weights[j], jnp.float32).astype(jnp.bfloat16)
    tail = jnp.where(row < 2, weights[0], weights[1]).astype(jnp.bfloat16)
    first_ref[:, cells:] = tail
    second_ref[:, cells:] = tail

    def step(g):
        v = [orbitals_ref[j, :, columns(g)].astype(jnp.float32) for j in range(2)]

        def rows(a, b):
            return jnp.concatenate([v[0][a : a + 1], v[0][b : b + 1], v[1][a : a + 1], v[1][b : b + 1]], axis=0)

        high, leading = rows(planes - 1, planes - 2), rows(1, 0)
        first_ref[:, columns(g)] = jnp.where(even, high, leading).astype(jnp.bfloat16)
        second_ref[:, columns(g)] = jnp.where(even, leading, high).astype(jnp.bfloat16)

    sweep(step, cells // LANES, 8)


def neighbour_table():
    size = (2 * LANES, 2 * LANES)
    a, b = (lax.broadcasted_iota(jnp.int32, size, d) for d in range(2))
    apart = jnp.abs(a - b)
    near = (apart == NZ) | ((apart == 1) & (a // NZ == b // NZ))
    return jnp.where(near, 1.0, 0.0).astype(jnp.bfloat16)


def visit_kernel(*refs):
    first = len(refs) == 6
    own_ref, visitor_ref = refs[:2]
    if first:
        out_ref, table_ref, rho, mid = refs[2:]
        table_ref[...] = neighbour_table()
    else:
        running_ref, table_ref, out_ref, rho, mid = refs[2:]
    groups = out_ref.shape[2] // LANES
    low = iotas()[1] < NZ
    zero = jnp.zeros(SHAPE, jnp.float32)
    weight = []
    for j in range(2):
        w = visitor_ref[j, :, groups * LANES :].astype(jnp.float32)
        weight.append(w[:8] * -lead)
    for ref in (rho, mid):
        for at in range(4):
            for e in range(2):
                ref[0, at_row(at, e), :] = zero
                ref[groups + 1, at_row(at, e), :] = zero

    def stencils(ref, g0, count):
        rows = []
        for q in range(0, count, 2):
            for at in range(4):
                both = [ref[g0 + q + 1 + h, pl.ds(24 * at + 8, 16), :] for h in range(2)]
                rows.append(jnp.concatenate(both, axis=1))
        v = jnp.concatenate(rows, axis=0)
        coarse = v.astype(jnp.bfloat16)
        fine = (v - coarse.astype(jnp.float32)).astype(jnp.bfloat16)
        table = table_ref[...]
        inner = jnp.dot(coarse, table, preferred_element_type=jnp.float32)
        inner = inner + jnp.dot(fine, table, preferred_element_type=jnp.float32)
        result = {}
        for q in range(0, count, 2):
            for at in range(4):
                for e in range(2):
                    g = g0 + q + 1
                    rows = at_row(at, e)
                    outer = lanes_by(jnp.where(low, ref[g + 2, rows, :], ref[g - 1, rows, :]), NZ)
                    for h in range(2):
                        x = ref[g + h, at_row(at, e, -1), :] + ref[g + h, at_row(at, e, 1), :]
                        r = 32 * q + 16 * at + 8 * e
                        yz = inner[r : r + 8, LANES * h : LANES * h + LANES]
                        edge = jnp.where(low if h == 0 else ~low, outer, 0.0)
                        result[q + h, at, e] = (x + edge) + yz
        return result

    def step_rho(g):
        own = [planes_of(own_ref, i, g) for i in range(2)]
        vis = [planes_of(visitor_ref, j, g) for j in range(2)]
        for n in range(5):
            rho[g + 1, pl.ds(24 * n, 8), :] = zero
            mid[g + 1, pl.ds(24 * n, 8), :] = zero
        for at, (i, j) in enumerate(PAIRS):
            for e in range(2):
                rho[g + 1, at_row(at, e), :] = own[i][e] * vis[j][e]

    def step_mid(n):
        g0 = n * CHUNK
        nb = stencils(rho, g0, CHUNK)
        for (k, at, e), s in nb.items():
            mid[g0 + k + 1, at_row(at, e), :] = rho[g0 + k + 1, at_row(at, e), :] * slope + s

    def step_out(n):
        g0 = n * CHUNK
        nb = stencils(mid, g0, CHUNK)
        for k in range(CHUNK):
            g = g0 + k
            vis = [planes_of(visitor_ref, j, g) for j in range(2)]
            for i in range(2):
                for e in range(2):
                    total = None
                    for at in range(4):
                        if PAIRS[at][0] == i:
                            pot = rho[g + 1, at_row(at, e), :] * base + nb[k, at, e]
                            j = PAIRS[at][1]
                            term = (weight[j] * vis[j][e]) * pot
                            total = term if total is None else total + term
                    if not first:
                        total = total + running_ref[i, 8 * e : 8 * e + 8, columns(g)]
                    out_ref[i, 8 * e : 8 * e + 8, columns(g)] = total

    sweep(step_rho, groups, UNROLL_RHO)
    sweep(step_mid, groups // CHUNK, 1)
    sweep(step_out, groups // CHUNK, 1)


def edge_kernel(own_ref, own_halo_ref, *rest):
    out_ref, total_ref, rho, scaled_edge, packed, natural, sems = rest[-7:]
    running_ref = rest[-8]
    visitors = rest[: (len(rest) - 8) // 2]
    halos = rest[(len(rest) - 8) // 2 : -8]
    groups = out_ref.shape[2] // LANES
    row, lane = iotas()
    high, has_left, has_right = lane >= NZ, lane % NZ != 0, lane % NZ != NZ - 1
    zero = jnp.zeros(SHAPE, jnp.float32)
    inside = own_halo_ref[:, groups * LANES :].astype(jnp.float32) > 0.0
    near = (row == 0) | (row == 2) | (row == 5) | (row == 7)
    even_row = row % 2 == 0
    upper = row % 4 < 2

    def swap(v):
        return jnp.where(upper, rows_by(v, -2), rows_by(v, 2))

    def beside(v):
        return jnp.where(even_row, rows_by(v, -1), rows_by(v, 1))

    def edges(ref, g):
        a0, a1 = planes_of(ref, 0, g)
        b0, b1 = planes_of(ref, 1, g)
        return jnp.where(row < 2, a0, jnp.where(row < 4, rows_by(b0, 2), jnp.where(row < 6, rows_by(a1, -2), b1)))

    weight = []
    for ref in visitors:
        w0 = ref[0, :, groups * LANES :].astype(jnp.float32)[:8]
        w1 = ref[1, :, groups * LANES :].astype(jnp.float32)[:8]
        weight.append(jnp.where(upper, w0, w1) * -lead)
    for n in range(len(visitors)):
        rho[0, n] = zero
        rho[groups + 1, n] = zero

    def step_rho(g):
        oh = own_halo_ref[:, columns(g)].astype(jnp.float32)
        oh_beside, swapped_beside = beside(oh), beside(swap(oh))
        oe = edges(own_ref, g)
        oh_packed = jnp.where(near, oh, swapped_beside)
        oe_packed = jnp.where(inside, jnp.where(near, oe, beside(swap(oe))), 0.0)
        first_sum, second_sum = None, None
        for n, (ref, halo_ref) in enumerate(zip(visitors, halos)):
            vh = halo_ref[:, columns(g)].astype(jnp.float32)
            ve = edges(ref, g)
            vh_beside = beside(vh)
            rho[g + 1, n] = oh_packed * jnp.where(near, vh, vh_beside)
            ve_packed = jnp.where(near, ve, beside(ve))
            we_packed = weight[n] * ve_packed
            scaled_edge[g, n] = we_packed
            a, b = (weight[n] * ve) * vh_beside, we_packed * ve_packed
            first_sum = a if first_sum is None else first_sum + a
            second_sum = b if second_sum is None else second_sum + b
        natural[g] = first_sum * oh_beside + swap(first_sum * swapped_beside)
        packed[g] = second_sum * oe_packed

    def step_out(g):
        total = packed[g]
        for n in range(len(visitors)):
            v = rho[g + 1, n]
            left = jnp.where(has_left, lanes_by(v, 1), 0.0)
            right = jnp.where(has_right, lanes_by(v, -1), 0.0)
            about = lanes_by(v + jnp.where(high, rho[g, n], rho[g + 2, n]), NZ)
            t = about + (left + right)
            total = total + scaled_edge[g, n] * (v * slope + (t + t))
        total = natural[g] + jnp.where(near, total, 0.0) + swap(beside(jnp.where(near, 0.0, total)))
        cols = pl.ds(g * LANES, LANES)
        for i in range(2):
            low_planes = total if i == 0 else rows_by(total, -2)
            total_ref[i, :8, cols] = running_ref[i, :8, cols] + jnp.where(row < 2, low_planes, 0.0)
            high_planes = rows_by(total, 2) if i == 0 else total
            total_ref[i, 8:, cols] = running_ref[i, 8:, cols] + jnp.where(row >= 6, high_planes, 0.0)

    sweep(step_rho, groups, 16)
    parts = sems.shape[0]
    width = groups // parts
    copies = []
    for c in range(parts):
        for k in range(width):
            step_out(c * width + k)
        cols = pl.ds(c * width * LANES, width * LANES)
        copy = pltpu.make_async_copy(total_ref.at[:, :, cols], out_ref.at[:, :, cols], sems.at[c])
        copy.start()
        copies.append(copy)
    for copy in copies:
        copy.wait()


VMEM = pl.BlockSpec(memory_space=pltpu.VMEM)


def in_vmem(x):
    return pltpu.with_memory_space_constraint(x, pltpu.VMEM)


def prepare(orbitals, occupation, even_of):
    cells = orbitals.shape[2]
    return pl.pallas_call(
        lambda *refs: prepare_kernel(*refs, even_of=even_of),
        out_shape=[
            pltpu.VMEM((*orbitals.shape[:2], cells + LANES), orbitals.dtype),
            pltpu.VMEM((4, cells + LANES), orbitals.dtype),
            pltpu.VMEM((4, cells + LANES), orbitals.dtype),
        ],
        in_specs=[VMEM, pl.BlockSpec(memory_space=pltpu.SMEM)],
        out_specs=[VMEM] * 3,
        name="prepare",
    )(orbitals, occupation)


def visit(own, visitor, running=None, table=None):
    shape = (*own.shape[:2], own.shape[2] - LANES)
    groups = shape[2] // LANES
    first = running is None
    operands = [in_vmem(x) for x in (own, visitor) + (() if first else (running, table))]
    held = pltpu.VMEM((groups + 2, 104, LANES), jnp.float32)
    out = pltpu.VMEM(shape, jnp.float32)
    return pl.pallas_call(
        visit_kernel,
        out_shape=[out, pltpu.VMEM((2 * LANES, 2 * LANES), jnp.bfloat16)] if first else out,
        in_specs=[VMEM] * len(operands),
        out_specs=[VMEM] * 2 if first else VMEM,
        scratch_shapes=[held, held],
        name="visit",
    )(*operands)


def finish(own, own_halo, visitors, halos, running):
    groups = running.shape[2] // LANES
    count = len(visitors)
    operands = [in_vmem(x) for x in (own, own_halo, *visitors, *halos, running)]
    return pl.pallas_call(
        edge_kernel,
        out_shape=jax.ShapeDtypeStruct(running.shape, jnp.float32),
        in_specs=[VMEM] * len(operands),
        out_specs=pl.BlockSpec(memory_space=pl.ANY),
        scratch_shapes=[
            pltpu.VMEM(running.shape, jnp.float32),
            pltpu.VMEM((groups + 2, count, *SHAPE), jnp.float32),
            pltpu.VMEM((groups, count, *SHAPE), jnp.float32),
            pltpu.VMEM((groups, *SHAPE), jnp.float32),
            pltpu.VMEM((groups, *SHAPE), jnp.float32),
            pltpu.SemaphoreType.DMA((4,)),
        ],
        name="finish",
    )(*operands)


def from_two_back(array):
    size = lax.axis_size("band")
    return lax.ppermute(array, "band", [(i, (i + 2) % size) for i in range(size)])


def across_pair_and_three(array):
    size = lax.axis_size("band")
    return lax.ppermute(array, "band", [(i, (i + 1 + 2 * (i % 2)) % size) for i in range(size)])


def swapped_in_pair(array):
    size = lax.axis_size("band")
    return lax.ppermute(array, "band", [(i, i ^ 1) for i in range(size)])


def per_device(orbitals, occupation):
    size = lax.axis_size("slab")
    even = lax.axis_index("slab") % 2 == 0
    wide, first, second = prepare(orbitals, occupation, lambda: lax.axis_index("slab") % 2 == 0)
    beside_second = lax.ppermute(second, "slab", [(i, ((i - 1) ^ 1) + 1) for i in range(1, size - 1)])
    beside_first = lax.ppermute(first, "slab", [(i, i ^ 1) for i in range(size)])
    two_back = from_two_back(wide)
    other = across_pair_and_three(wide)
    swapped = swapped_in_pair(two_back)
    halo = jnp.concatenate([jnp.where(even, beside_second, beside_first), jnp.where(even, beside_first, beside_second)], axis=0)
    halo_two = from_two_back(halo)
    halo_other = across_pair_and_three(halo)
    halo_swapped = swapped_in_pair(halo_two)
    running, table = visit(wide, wide)
    running = visit(wide, two_back, running, table)
    running = visit(wide, swapped, running, table)
    running = visit(wide, other, running, table)
    return finish(wide, halo, (wide, two_back, swapped, other), (halo, halo_two, halo_swapped, halo_other), running)


def solution(mesh):
    return jax.shard_map(
        per_device,
        mesh=mesh,
        in_specs=(P("band", "slab", None), P("band")),
        out_specs=P("band", "slab", None),
        check_vma=False,
    )
```
